256 devices in a mesh: section: 4 (over x), depth: 64 (over z, y, core).
Axes of the slice: x: 4, y: 4, z: 8, core: 2. Of those that a mesh axis runs over, the one named last changes fastest.
Arguments:
- activations: float32 [4, 4, 128, 64, 256], P('section', None, 'depth'), may hold values from -6 to 6
- filters: float32 [4, 27, 64, 64], P('section'), may hold values from -0.15625 to 0.15625
- cotangent: float32 [4, 128, 64, 256], P(None, 'depth'), may hold values from -6 to 6
Outputs:
- input_grads: float32 [4, 4, 128, 64, 256], P('section', None, 'depth')
- filter_grads: float32 [4, 27, 64, 64], P('section')
The draws below stay inside these ranges and needn't reach their ends.
All inputs are finite; a program needn't handle non-finite values.
Results may differ from the reference program's by a relative error of at most 0.0003.
Values sent between devices are 32-bit elements; how exact they have to be, the bound alone decides.
A program may use at most 128 MiB of HBM per device.

```python
import math
import jax
import jax.numpy as jnp
from jax import lax

C = 64
H = 16
W = 16
MB = 4
SECTIONS = 4
DEPTH = 128
N_SECTION = 4


def level_of(rng, shape, split, least, largest):
    gain, own = 1.0, jax.random.fold_in(rng, 6)
    for dim, blocks in split:
        draws = jnp.exp(jax.random.uniform(jax.random.fold_in(own, dim), (blocks,), jnp.float32, least / len(split), largest / len(split)))
        gain = gain * jnp.repeat(draws, shape[dim] // blocks).reshape([-1 if axis == dim else 1 for axis in range(len(shape))])
    return gain


def gaussian(stream_key, dims, spread, bound, shards=(), dtype=jnp.bfloat16):
    loudness = level_of(stream_key, dims, shards, -0.22, 0.18) if shards else 1.0
    values = jax.random.normal(stream_key, dims, jnp.float32) * spread * loudness
    return jnp.minimum(jnp.maximum(values, -bound), bound).astype(dtype)


def setup_inputs(seed: int = 0) -> dict:
    streams_of = jax.random.split(jax.random.key(seed), 4)
    return {
        "activations": gaussian(streams_of[0], (SECTIONS, MB, DEPTH, C, H * W), 1.0, 6.0, ((0, 4), (2, 64)), jnp.float32),
        "filters": gaussian(streams_of[1], (SECTIONS, 27, C, C), (27 * C) ** -0.5, 0.15625, ((0, 4),), jnp.float32),
        "cotangent": gaussian(streams_of[2], (MB, DEPTH, C, H * W), 1.0, 6.0, ((1, 64),), jnp.float32),
    }


def convolve(volume, kernel_taps):
    depth_cells, channels, columns = volume.shape
    volume_grid = volume.reshape(1, depth_cells, channels, H, W).transpose(0, 2, 1, 3, 4)
    kernel = kernel_taps.reshape(3, 3, 3, channels, channels).transpose(3, 4, 0, 1, 2)
    result = lax.conv_general_dilated(volume_grid, kernel, (1, 1, 1), ((1, 1), (1, 1), (1, 1)), dimension_numbers=('NCDHW', 'OIDHW', 'NCDHW'), precision=lax.Precision.HIGHEST)
    return result[0].transpose(1, 0, 2, 3).reshape(depth_cells, channels, columns)

def silu_slope(preact):
    sigmoid_value = jax.nn.sigmoid(preact)
    return sigmoid_value * (1.0 + preact * (1.0 - sigmoid_value))

def reference(activations, filters, cotangent):
    upstream = [cotangent[micro_index] for micro_index in range(MB)]
    grad_layers = [None] * N_SECTION
    filter_layers = [None] * N_SECTION
    for layer_index in reversed(range(N_SECTION)):
        summed = jnp.zeros(filters.shape[1:], jnp.float32)
        outgoing = []
        for micro_index in range(MB):
            preact, pullback = jax.vjp(convolve, activations[layer_index, micro_index], filters[layer_index])
            slopes = upstream[micro_index] * silu_slope(preact)
            backward, filter_term = pullback(slopes)
            summed = summed + filter_term
            outgoing.append(backward)
        grad_layers[layer_index] = jnp.stack(outgoing)
        filter_layers[layer_index] = summed
        upstream = outgoing
    scaling = 1.0 / math.sqrt(MB * DEPTH * H * W)
    return (jnp.stack(grad_layers), jnp.stack(filter_layers) * scaling)
```

```python
import functools
import math

import jax
import jax.numpy as jnp
from jax import lax
from jax.experimental import pallas as pl
from jax.experimental.pallas import tpu as pltpu
from jax.sharding import PartitionSpec as P

W = 16
MESH = pl.DeviceIdType.MESH
F32 = jnp.float32
BF16 = jnp.bfloat16


def split(x):
    hi = x.astype(BF16)
    lo = (x - hi.astype(F32)).astype(BF16)
    return hi, lo


def tap_mask(row_step, col_step, cells):
    at = lax.broadcasted_iota(jnp.int32, (1, cells), 1)
    row = at // W + row_step
    col = at % W + col_step
    return (row >= 0) & (row < cells // W) & (col >= 0) & (col < W)


def shifted(x, row_step, col_step):
    if row_step == 0 and col_step == 0:
        return x
    cells = x.shape[-1]
    turned = pltpu.roll(x, (-(row_step * W + col_step)) % cells, 1)
    return jnp.where(tap_mask(row_step, col_step, cells), turned, 0.0)


def kernel(
    grid,
    act, filt, cot, igrad, fgrad,
    wf, wb, halo_a, halo_s, x3, s3, taps, slope, sf, relay, turned, fsum,
    ar, r1, r2, r3, gathered,
    ha_send, ha_recv, hs_send, hs_recv, rel_send, rel_recv,
    c_send, c_recv, y_send, y_recv, z_send, z_recv,
    gz_send, gz_recv, gy_send, gy_recv, gc_send, gc_recv,
):
    nz, ny, nc = grid
    sections = lax.axis_size("section")
    slabs = lax.axis_size("depth")
    s = lax.axis_index("section")
    d = lax.axis_index("depth")
    micro = act.shape[1]
    C = act.shape[3]
    cells = act.shape[4]
    z, y, c = d // (ny * nc), (d // nc) % ny, d % nc
    top = s == sections - 1
    T = 9 * C

    def at_depth(zz, yy, cc):
        return {"depth": (zz * ny + yy) * nc + cc}

    lower, upper = {"depth": d - 1}, {"depth": d + 1}
    y_peers = [at_depth(z, (y + j) % ny, c) for j in range(1, ny)]
    z_peers = [at_depth((z + j) % nz, y, c) for j in range(1, nz)]
    c_peers = [at_depth(z, y, (c + j) % nc) for j in range(1, nc)]

    barrier = pltpu.get_barrier_semaphore()

    def greet(device):
        pl.semaphore_signal(barrier, inc=1, device_id=device, device_id_type=MESH)

    pl.when(d > 0)(lambda: greet(lower))
    pl.when(d < slabs - 1)(lambda: greet(upper))
    pl.when(s > 0)(lambda: greet({"section": s - 1}))
    pl.when(s < sections - 1)(lambda: greet({"section": s + 1}))
    for peer in y_peers + z_peers + c_peers:
        greet(peer)
    expected = (
        (d > 0).astype(jnp.int32)
        + (d < slabs - 1).astype(jnp.int32)
        + (s > 0).astype(jnp.int32)
        + (s < sections - 1).astype(jnp.int32)
        + (nz + ny + nc - 3)
    )
    pl.semaphore_wait(barrier, expected)

    def remote(src, dst, send, recv, device):
        return pltpu.make_async_remote_copy(
            src_ref=src, dst_ref=dst, send_sem=send, recv_sem=recv, device_id=device, device_id_type=MESH
        )

    def face_a(m, side):
        plane, to = (1, upper) if side == 0 else (0, lower)
        return remote(act.at[0, m, plane], halo_a.at[side, m], ha_send.at[side, m], ha_recv.at[side, m], to)

    def face_s(m, side):
        plane, to = (1, upper) if side == 0 else (0, lower)
        return remote(sf.at[m, plane], halo_s.at[side, m], hs_send.at[side, m], hs_recv.at[side, m], to)

    def pass_down(m):
        return remote(igrad.at[0, m], relay.at[m], rel_send.at[m], rel_recv.at[m], {"section": s - 1})

    for m in range(micro):
        pl.when(d > 0)(lambda m=m: face_a(m, 1).start())
        pl.when(d < slabs - 1)(lambda m=m: face_a(m, 0).start())

    none = jnp.zeros((C, C), F32)

    def prepare(t, carry):
        rows0 = pl.ds(pl.multiple_of(t * C, C), C)
        rows1 = pl.ds(pl.multiple_of(T + t * C, C), C)
        f = [filt[0, 9 * a + t] for a in range(3)]
        g = [filt[0, 26 - 9 * a - t].T for a in range(3)]
        for w, b in ((wf, f), (wb, g)):
            for rows, parts in ((rows0, [*b, none]), (rows1, [none, *b])):
                hi, lo = split(jnp.concatenate(parts, axis=1))
                w[rows, : 4 * C] = hi
                w[rows, 4 * C :] = lo
        return carry

    lax.fori_loop(0, 9, prepare, 0)
    fsum[...] = jnp.zeros_like(fsum)
    ar[...] = jnp.zeros_like(ar)

    E = 4 * C

    def put(buf, rows, x):
        hi, lo = split(x)
        lead = rows * C
        return hi, lo, pl.ds(lead, C), pl.ds(E + lead, C)

    def convolve(w, hi, lo, store):
        rhs = jnp.concatenate([hi, hi, lo], axis=0)
        for j in range(2):
            w_hi, w_lo = w[j * T : (j + 1) * T, :E], w[j * T : (j + 1) * T, E:]
            lhs = jnp.concatenate([w_hi, w_lo, w_hi], axis=1)
            taps[j * T : (j + 1) * T, :] = jnp.dot(lhs, rhs, preferred_element_type=F32)
        for j in range(2):
            total = taps[j * T + 4 * C : j * T + 5 * C, :]
            for t in (0, 1, 2, 3, 5, 6, 7, 8):
                total = total + shifted(taps[j * T + t * C : j * T + (t + 1) * C, :], t // 3 - 1, t % 3 - 1)
            store(j, total)

    def preact(m):
        for j in range(2):
            hi, lo = split(act[0, m, j])
            x3[m, (j + 1) * C : (j + 2) * C, :] = hi
            x3[m, E + (j + 1) * C : E + (j + 2) * C, :] = lo
        for side, has in ((0, d > 0), (1, d < slabs - 1)):
            first = 3 * C * side

            @pl.when(has)
            def _():
                face_a(m, side).wait_recv()
                hi, lo = split(halo_a[side, m])
                x3[m, first : first + C, :] = hi
                x3[m, E + first : E + first + C, :] = lo

            @pl.when(jnp.logical_not(has))
            def _():
                x3[m, first : first + C, :] = jnp.zeros((C, cells), BF16)
                x3[m, E + first : E + first + C, :] = jnp.zeros((C, cells), BF16)

        def store(j, total):
            sg = 1.0 / (1.0 + jnp.exp(-total))
            slope[m, j] = sg * (1.0 + total * (1.0 - sg))

        convolve(wf, x3[m, :E, :], x3[m, E:, :], store)

    def first_preacts(m, carry):
        preact(m)
        return carry

    lax.fori_loop(0, jnp.where(top, 1, micro), first_preacts, 0)

    def backward(m, carry):
        @pl.when(top)
        def _():
            sf[m] = cot[m] * slope[m]

        @pl.when(jnp.logical_not(top))
        def _():
            remote(igrad.at[0, m], relay.at[m], rel_send.at[m], rel_recv.at[m], {"section": s}).wait_recv()
            sf[m] = relay[m] * slope[m]

        for j in range(2):
            hi, lo = split(sf[m, j])
            s3[(j + 1) * C : (j + 2) * C, :] = hi
            s3[E + (j + 1) * C : E + (j + 2) * C, :] = lo
        pl.when(d > 0)(lambda: face_s(m, 1).start())
        pl.when(d < slabs - 1)(lambda: face_s(m, 0).start())

        for t in range(9):
            for j in range(2):
                hi, lo = split(shifted(sf[m, j], 1 - t // 3, 1 - t % 3))
                turned[t * C : (t + 1) * C, 2 * j * cells : (2 * j + 1) * cells] = hi
                turned[t * C : (t + 1) * C, (2 * j + 1) * cells : (2 * j + 2) * cells] = lo
        lhs = [turned[:, i * cells : (i + 1) * cells] for i in (0, 1, 0, 2, 3, 2)]
        rhs = [x3[m, first : first + 3 * C, :] for first in (0, 0, E, C, C, E + C)]
        fsum[...] += lax.dot_general(
            jnp.concatenate(lhs, axis=1),
            jnp.concatenate(rhs, axis=1),
            (((1,), (1,)), ((), ())),
            preferred_element_type=F32,
        )

        pl.when(top & (m < micro - 1))(lambda: preact(jnp.minimum(m + 1, micro - 1)))

        for side, has in ((0, d > 0), (1, d < slabs - 1)):
            first = 3 * C * side

            @pl.when(has)
            def _():
                face_s(m, side).wait_recv()
                hi, lo = split(halo_s[side, m])
                s3[first : first + C, :] = hi
                s3[E + first : E + first + C, :] = lo

            @pl.when(jnp.logical_not(has))
            def _():
                s3[first : first + C, :] = jnp.zeros((C, cells), BF16)
                s3[E + first : E + first + C, :] = jnp.zeros((C, cells), BF16)

        def store(j, total):
            igrad[0, m, j] = total

        convolve(wb, s3[:E, :], s3[E:, :], store)
        pl.when(s > 0)(lambda: pass_down(m).start())
        return carry

    lax.fori_loop(0, micro, backward, 0)

    chunks = nz * ny * nc
    rows = ar.shape[1]
    half = T // 2
    ar[: T // rows] = fsum[:, :128].reshape(T // rows, rows, 128)
    ar[T // rows : (T + half) // rows] = jnp.concatenate(
        [fsum[:half, 128:], fsum[half:, 128:]], axis=1
    ).reshape(half // rows, rows, 128)

    per_c, per_y = nz * ny, nz

    def block_c(cc):
        return pl.ds(cc * per_c, per_c)

    def block_y(yy):
        return pl.ds(c * per_c + yy * per_y, per_y)

    mine = c * per_c + y * per_y + z

    to_c = [
        remote(ar.at[block_c((c + j) % nc)], r1.at[j - 1], c_send.at[j - 1], c_recv.at[j - 1], c_peers[j - 1])
        for j in range(1, nc)
    ]
    for copy in to_c:
        copy.start()
    for copy in to_c:
        copy.wait_recv()
    for j in range(nc - 1):
        ar[block_c(c)] += r1[j]

    to_y = [
        remote(ar.at[block_y((y + j) % ny)], r2.at[j - 1], y_send.at[j - 1], y_recv.at[j - 1], y_peers[j - 1])
        for j in range(1, ny)
    ]
    for copy in to_y:
        copy.start()
    for copy in to_y:
        copy.wait_recv()
    total = ar[block_y(y)]
    for j in range(ny - 1):
        total = total + r2[j]
    ar[block_y(y)] = total

    to_z = [
        remote(
            ar.at[c * per_c + y * per_y + (z + j) % nz], r3.at[j - 1], z_send.at[j - 1], z_recv.at[j - 1], z_peers[j - 1]
        )
        for j in range(1, nz)
    ]
    for copy in to_z:
        copy.start()
    for copy in to_z:
        copy.wait_recv()
    total = ar[mine]
    for j in range(nz - 1):
        total = total + r3[j]
    scaling = 1.0 / math.sqrt(micro * 2 * slabs * cells)
    gathered[mine] = total * scaling

    out_z = [
        remote(gathered.at[mine], gathered.at[mine], gz_send.at[j], gz_recv.at[j], z_peers[j]) for j in range(nz - 1)
    ]
    for copy in out_z:
        copy.start()
    for copy in out_z:
        copy.wait_recv()
    out_y = [
        remote(gathered.at[block_y(y)], gathered.at[block_y(y)], gy_send.at[j], gy_recv.at[j], y_peers[j])
        for j in range(ny - 1)
    ]
    for copy in out_y:
        copy.start()
    for copy in out_y:
        copy.wait_recv()
    out_c = [
        remote(gathered.at[block_c(c)], gathered.at[block_c(c)], gc_send.at[j], gc_recv.at[j], c_peers[j])
        for j in range(nc - 1)
    ]
    for copy in out_c:
        copy.start()
    for copy in out_c:
        copy.wait_recv()

    done = gathered[: (T + half) // rows].reshape(T + half, 128)
    last = jnp.concatenate([done[T:, :C], done[T:, C:]], axis=0)
    for t in range(9):
        block = done[t * C : (t + 1) * C, :]
        fgrad[0, t] = block[:, :C]
        fgrad[0, 9 + t] = block[:, C:]
        fgrad[0, 18 + t] = last[t * C : (t + 1) * C, :]

    for copy in to_c + to_y + to_z + out_z + out_y + out_c:
        copy.wait_send()
    for m in range(micro):
        for side, has in ((1, d > 0), (0, d < slabs - 1)):
            pl.when(has)(lambda m=m, side=side: face_a(m, side).wait_send())
            pl.when(has)(lambda m=m, side=side: face_s(m, side).wait_send())
        pl.when(s > 0)(lambda m=m: pass_down(m).wait_send())


def per_device(grid, activations, filters, cotangent):
    micro, planes, C, cells = activations.shape[1:]
    nz, ny, nc = grid
    chunks = nz * ny * nc
    rows = -(-(27 * C * C) // (128 * 8 * chunks)) * 8
    rows = next(r for r in (8, 16, 32, 48, 96, 144, 288) if r >= rows)
    dma = pltpu.SemaphoreType.DMA
    vmem = pl.BlockSpec(memory_space=pltpu.VMEM)
    plane = (C, cells)
    return pl.pallas_call(
        functools.partial(kernel, grid),
        out_shape=(
            jax.ShapeDtypeStruct(activations.shape, F32),
            jax.ShapeDtypeStruct(filters.shape, F32),
        ),
        in_specs=[vmem] * 3,
        out_specs=(vmem, vmem),
        scratch_shapes=[
            pltpu.VMEM((18 * C, 8 * C), BF16),
            pltpu.VMEM((18 * C, 8 * C), BF16),
            pltpu.VMEM((2, micro, *plane), F32),
            pltpu.VMEM((2, micro, *plane), F32),
            pltpu.VMEM((micro, 8 * C, cells), BF16),
            pltpu.VMEM((8 * C, cells), BF16),
            pltpu.VMEM((18 * C, cells), F32),
            pltpu.VMEM((micro, planes, *plane), F32),
            pltpu.VMEM((micro, planes, *plane), F32),
            pltpu.VMEM((micro, planes, *plane), F32),
            pltpu.VMEM((9 * C, 4 * cells), BF16),
            pltpu.VMEM((9 * C, 3 * C), F32),
            pltpu.VMEM((chunks, rows, 128), F32),
            pltpu.VMEM((max(nc - 1, 1), nz * ny, rows, 128), F32),
            pltpu.VMEM((max(ny - 1, 1), nz, rows, 128), F32),
            pltpu.VMEM((max(nz - 1, 1), rows, 128), F32),
            pltpu.VMEM((chunks, rows, 128), F32),
            dma((2, micro)), dma((2, micro)), dma((2, micro)), dma((2, micro)), dma((micro,)), dma((micro,)),
            dma((max(nc - 1, 1),)), dma((max(nc - 1, 1),)), dma((max(ny - 1, 1),)), dma((max(ny - 1, 1),)),
            dma((max(nz - 1, 1),)), dma((max(nz - 1, 1),)), dma((max(nz - 1, 1),)), dma((max(nz - 1, 1),)),
            dma((max(ny - 1, 1),)), dma((max(ny - 1, 1),)), dma((max(nc - 1, 1),)), dma((max(nc - 1, 1),)),
        ],
        compiler_params=pltpu.CompilerParams(
            collective_id=0, has_side_effects=True, vmem_limit_bytes=60 * 1024 * 1024
        ),
    )(activations, filters, cotangent)


def solution(mesh):
    slabs = mesh.shape["depth"]
    grid = (slabs // 8, 4, 2) if slabs >= 32 else (slabs // 4, 2, 2)
    return jax.shard_map(
        functools.partial(per_device, grid),
        mesh=mesh,
        in_specs=(
            P("section", None, "depth", None, None),
            P("section", None, None, None),
            P(None, "depth", None, None),
        ),
        out_specs=(P("section", None, "depth", None, None), P("section", None, None, None)),
        check_vma=False,
    )
```

```python
import functools
import math

import jax
import jax.numpy as jnp
from jax import lax
from jax.experimental import pallas as pl
from jax.experimental.pallas import tpu as pltpu
from jax.sharding import PartitionSpec as P

W = 16
MESH = pl.DeviceIdType.MESH
F32 = jnp.float32
BF16 = jnp.bfloat16


def split(x):
    hi = x.astype(BF16)
    lo = (x - hi.astype(F32)).astype(BF16)
    return hi, lo


def tap_mask(row_step, col_step, cells):
    at = lax.broadcasted_iota(jnp.int32, (1, cells), 1)
    row = at // W + row_step
    col = at % W + col_step
    return (row >= 0) & (row < cells // W) & (col >= 0) & (col < W)


def shifted(x, row_step, col_step):
    if row_step == 0 and col_step == 0:
        return x
    cells = x.shape[-1]
    turned = pltpu.roll(x, (-(row_step * W + col_step)) % cells, 1)
    return jnp.where(tap_mask(row_step, col_step, cells), turned, 0.0)


def kernel(
    grid,
    act_hbm, filt_hbm, cot_hbm, igrad, fgrad,
    act, filt, cot, wf, wb, halo_a, halo_s, x3, s3, taps, slope, sf, relay, turned, fsum,
    ar, r1, r2, r3, gathered,
    ha_send, ha_recv, hs_send, hs_recv, rel_send, rel_recv,
    c_send, c_recv, y_send, y_recv, z_send, z_recv,
    gz_send, gz_recv, gy_send, gy_recv, gc_send, gc_recv, in_sem, known,
):
    nz, ny, nc = grid
    sections = lax.axis_size("section")
    slabs = lax.axis_size("depth")
    s = lax.axis_index("section")
    d = lax.axis_index("depth")
    micro = act.shape[1]
    C = act.shape[3]
    cells = act.shape[4]
    z, y, c = d // (ny * nc), (d // nc) % ny, d % nc
    top = s == sections - 1
    T = 9 * C
    E = 4 * C
    LO = 5 * C

    def at_depth(zz, yy, cc):
        return {"depth": (zz * ny + yy) * nc + cc}

    outer, inner = c, 1 - c
    across = d - 1 + 2 * c
    has_outer = (across >= 0) & (across < slabs)
    far, near = {"depth": across}, {"depth": d + 1 - 2 * c}
    y_peers = [at_depth(z, (y + j) % ny, c) for j in range(1, ny)]
    z_peers = [at_depth((z + j) % nz, y, c) for j in range(1, nz)]

    loads = [
        pltpu.make_async_copy(src, dst, in_sem.at[k])
        for k, (src, dst) in enumerate(((act_hbm, act), (filt_hbm, filt), (cot_hbm, cot)))
    ]
    for load in loads:
        load.start()

    barrier = pltpu.get_barrier_semaphore()

    def greet(device):
        pl.semaphore_signal(barrier, inc=1, device_id=device, device_id_type=MESH)

    pl.when(has_outer)(lambda: greet(far))
    pl.when(s > 0)(lambda: greet({"section": s - 1}))
    pl.when(s < sections - 1)(lambda: greet({"section": s + 1}))
    y_sides = [at_depth(z, (y + j) % ny, c) for j in (1, ny - 1)]
    z_sides = [at_depth((z + j) % nz, y, c) for j in (1, nz - 1)]
    for peer in [near] + y_sides + z_sides:
        greet(peer)
    expected = (
        has_outer.astype(jnp.int32)
        + (s > 0).astype(jnp.int32)
        + (s < sections - 1).astype(jnp.int32)
        + 5
    )

    def remote(src, dst, send, recv, device):
        return pltpu.make_async_remote_copy(
            src_ref=src, dst_ref=dst, send_sem=send, recv_sem=recv, device_id=device, device_id_type=MESH
        )

    def face_a(m, which):
        plane, to = ((outer, far), (inner, near))[which]
        return remote(act.at[0, m, plane], halo_a.at[which, m], ha_send.at[which], ha_recv.at[which, m], to)

    def face_s(m, which):
        plane, to = ((outer, far), (inner, near))[which]
        return remote(sf.at[m, plane], halo_s.at[which, m], hs_send.at[which], hs_recv.at[which, m], to)

    def pass_down(m, which, to=None):
        plane = (outer, inner)[which]
        return remote(
            igrad.at[0, m, plane], relay.at[m, plane], rel_send.at[which], rel_recv.at[which, m],
            {"section": s - 1 if to is None else to},
        )

    def every(buf, send, recv):
        return remote(buf, buf, send, recv, near)

    def lead(plane):
        return pl.multiple_of(plane * C, C)

    def put(buf, m, plane, x):
        hi, lo = split(x)
        buf[m, pl.ds(lead(plane), C), :] = hi
        buf[m, pl.ds(LO + lead(plane), C), :] = lo

    def tell(r):
        for peer in z_sides + (y_sides if r == 0 else []):
            pl.semaphore_signal(known.at[r], inc=1, device_id=peer, device_id_type=MESH)

    def hear(r):
        pl.semaphore_wait(known.at[r], 4 if r == 0 else 2)

    def send_faces(m):
        pl.when(has_outer)(lambda: face_a(m, 0).start())
        face_a(m, 1).start()

    with jax.named_scope("load_act"):
        loads[0].wait()
    with jax.named_scope("barrier"):
        pl.semaphore_wait(barrier, expected)
    send_faces(0)
    tell(0)

    with jax.named_scope("prepare"):
        edge = jnp.zeros((C, cells), F32)
        for m in range(micro):
            for j in range(2):
                put(x3, m, j + 1, act[0, m, j])
            put(x3, m, 4, edge)
            put(s3, m, 4, edge)
            put(s3, m, 3 * c, edge)
            pl.when(jnp.logical_not(has_outer))(lambda m=m: put(x3, m, 3 * c, edge))
        fsum[...] = jnp.zeros_like(fsum)
        ar[...] = jnp.zeros_like(ar)
        none = jnp.zeros((C, C), F32)
        loads[1].wait()

        def prepare(t, carry):
            rows = pl.ds(pl.multiple_of(t * C, C), C)
            f = [filt[0, 9 * a + t] for a in range(3)]
            g = [filt[0, 26 - 9 * a - t].T for a in range(3)]
            for w, b in ((wf, f), (wb, g)):
                hi, lo = split(jnp.concatenate([*b, none], axis=1))
                w[rows, :E] = hi
                w[rows, E:] = lo
            return carry

        lax.fori_loop(0, 9, prepare, 0)
        loads[2].wait()

    def convolve(w, buf, m, j, slot):
        hi = buf[m, pl.ds(lead(j), E), :]
        lo = buf[m, pl.ds(LO + lead(j), E), :]
        lhs = jnp.concatenate([w[:, :E], w[:, E:], w[:, :E]], axis=1)
        taps[slot] = jnp.dot(lhs, jnp.concatenate([hi, hi, lo], axis=0), preferred_element_type=F32)
        total = taps[slot, 4 * C : 5 * C, :]
        for t in (0, 1, 2, 3, 5, 6, 7, 8):
            total = total + shifted(taps[slot, t * C : (t + 1) * C, :], t // 3 - 1, t % 3 - 1)
        return total

    def preact(m):
        @pl.when(has_outer)
        def _():
            with jax.named_scope("wait_ha"):
                face_a(m, 0).wait_recv()
            put(x3, m, 3 * c, halo_a[0, m])

        face_a(m, 1).wait_recv()
        put(x3, m, 3 * (1 - c), halo_a[1, m])

        @pl.when(m == 0)
        def _():
            for k in range(1, micro):
                send_faces(k)

        with jax.named_scope("pre_conv"):
            for j in range(2):
                total = convolve(wf, x3, m, j, j)
                sg = 1.0 / (1.0 + jnp.exp(-total))
                slope[m, j] = sg * (1.0 + total * (1.0 - sg))

    def first_preacts(m, carry):
        preact(m)
        return carry

    lax.fori_loop(0, jnp.where(top, 1, micro), first_preacts, 0)

    def take(m, which):
        plane = (outer, inner)[which]

        @pl.when(top)
        def _():
            sf[m, plane] = cot[m, plane] * slope[m, plane]

        @pl.when(jnp.logical_not(top))
        def _():
            with jax.named_scope("wait_relay"):
                pass_down(m, which, s).wait_recv()
            sf[m, plane] = relay[m, plane] * slope[m, plane]

        put(s3, m, plane + 1, sf[m, plane])
        if which == 0:
            pl.when(has_outer)(lambda: face_s(m, 0).start())
        else:
            face_s(m, 1).start()

    def filter_terms(m, which):
        plane = (outer, inner)[which]
        with jax.named_scope("fg"):
            for t in range(9):
                hi, lo = split(shifted(sf[m, plane], 1 - t // 3, 1 - t % 3))
                turned[which, t * C : (t + 1) * C, :cells] = hi
                turned[which, t * C : (t + 1) * C, cells:] = lo
            hi, lo = turned[which, :, :cells], turned[which, :, cells:]
            x_hi = x3[m, pl.ds(lead(plane), 3 * C), :]
            x_lo = x3[m, pl.ds(LO + lead(plane), 3 * C), :]
            fsum[...] += lax.dot_general(
                jnp.concatenate([hi, lo, hi], axis=1),
                jnp.concatenate([x_hi, x_hi, x_lo], axis=1),
                (((1,), (1,)), ((), ())),
                preferred_element_type=F32,
            )

    rows = ar.shape[1]
    half = T // 2
    per_c, per_y = nz * ny, nz

    def block_c(cc):
        return pl.ds(cc * per_c, per_c)

    def block_y(yy):
        return pl.ds(c * per_c + yy * per_y, per_y)

    def chunk(yy, j):
        return c * per_c + yy * per_y + (z + j) % nz

    def to_y(i, j):
        return remote(
            ar.at[chunk((y + i) % ny, j)], r2.at[i - 1, j], y_send, y_recv.at[i - 1, j], y_peers[i - 1]
        )

    def to_z(j):
        return remote(ar.at[chunk(y, j)], r3.at[j - 1], z_send, z_recv, z_peers[j - 1])

    by_distance = sorted(range(nz), key=lambda j: min(j, nz - j))
    to_c = remote(ar.at[block_c(1 - c)], r1, c_send, c_recv, near)

    def exchange():
        ar[: T // rows] = fsum[:, :128].reshape(T // rows, rows, 128)
        ar[T // rows : (T + half) // rows] = jnp.concatenate(
            [fsum[:half, 128:], fsum[half:, 128:]], axis=1
        ).reshape(half // rows, rows, 128)
        to_c.start()

    def start_sum():
        with jax.named_scope("to_c"):
            to_c.wait_recv()
        ar[block_c(c)] += r1[...]
        for j in reversed(by_distance):
            for i in range(1, ny):
                to_y(i, j).start()

    def backward(m, carry):
        pl.when(s == 0)(lambda: filter_terms(m, 0))
        take(m, 1)

        @pl.when(s == 0)
        def _():
            filter_terms(m, 1)
            pl.when(m == micro - 1)(exchange)

        with jax.named_scope("wait_hs1"):
            face_s(m, 1).wait_recv()
        put(s3, m, 3 * (1 - c), halo_s[1, m])
        with jax.named_scope("conv1"):
            igrad[0, m, inner] = convolve(wb, s3, m, inner, 1)
        pl.when((m == micro - 1) & (s == 0))(start_sum)

        @pl.when(m < micro - 1)
        def _():
            pl.when(top)(lambda: preact(m + 1))
            take(m + 1, 0)

        @pl.when(has_outer)
        def _():
            with jax.named_scope("wait_hs0"):
                face_s(m, 0).wait_recv()
            put(s3, m, 3 * c, halo_s[0, m])

        with jax.named_scope("conv0"):
            igrad[0, m, outer] = convolve(wb, s3, m, outer, 0)

        @pl.when(s > 0)
        def _():
            pass_down(m, 0).start()
            pass_down(m, 1).start()

        for r in range(3):

            @pl.when(m == r)
            def _():
                hear(r)
                if r < 2:
                    tell(r + 1)

        return carry

    take(0, 0)
    lax.fori_loop(0, micro, backward, 0)

    @pl.when(s > 0)
    def _():
        def terms(m, carry):
            filter_terms(m, 0)
            filter_terms(m, 1)
            return carry

        lax.fori_loop(0, micro, terms, 0)
        exchange()
        start_sum()

    for j in reversed(by_distance):
        with jax.named_scope("to_y"):
            for i in range(1, ny):
                to_y(i, j).wait_recv()
        total = ar[chunk(y, j)]
        for i in range(1, ny):
            total = total + r2[i - 1, j]
        if j > 0:
            ar[chunk(y, j)] = total
            to_z(j).start()
    with jax.named_scope("to_z"):
        every(r3, z_send, z_recv).wait_recv()
    for j in range(1, nz):
        total = total + r3[j - 1]
    scaling = 1.0 / math.sqrt(micro * 2 * slabs * cells)
    mine = chunk(y, 0)
    gathered[mine] = total * scaling

    def out_z(j):
        return remote(gathered.at[mine], gathered.at[mine], gz_send, gz_recv.at[j - 1], z_peers[j - 1])

    def out_y(i, j):
        at = chunk(y, nz - j)
        return remote(gathered.at[at], gathered.at[at], gy_send, gy_recv.at[i - 1], y_peers[i - 1])

    def out_c(i):
        at = block_y((y + i) % ny)
        return remote(gathered.at[at], gathered.at[at], gc_send, gc_recv, near)

    for j in reversed(by_distance):
        if j > 0:
            out_z(j).start()
    with jax.named_scope("out_z"):
        for j in by_distance:
            if j > 0:
                out_z(j).wait_recv()
            for i in range(1, ny):
                out_y(i, j).start()
    out_c(0).start()
    with jax.named_scope("out_y"):
        for i in range(1, ny):
            every(gathered.at[block_y((y + ny - i) % ny)], gy_send, gy_recv.at[i - 1]).wait_recv()
            out_c(ny - i).start()
    with jax.named_scope("out_c"):
        every(r1, gc_send, gc_recv).wait_recv()

    with jax.named_scope("unpack"):
        done = gathered[: (T + half) // rows].reshape(T + half, 128)
        last = jnp.concatenate([done[T:, :C], done[T:, C:]], axis=0)
        for t in range(9):
            block = done[t * C : (t + 1) * C, :]
            fgrad[0, t] = block[:, :C]
            fgrad[0, 9 + t] = block[:, C:]
            fgrad[0, 18 + t] = last[t * C : (t + 1) * C, :]

    to_c.wait_send()
    every(r2, y_send, c_recv).wait_send()
    every(r3, z_send, c_recv).wait_send()
    every(r3, gz_send, c_recv).wait_send()
    every(r2, gy_send, c_recv).wait_send()
    every(r1, gc_send, c_recv).wait_send()
    for which in range(2):

        def sent(which=which):
            every(halo_a.at[which], ha_send.at[which], c_recv).wait_send()
            every(halo_s.at[which], hs_send.at[which], c_recv).wait_send()

        pl.when(has_outer)(sent) if which == 0 else sent()
        pl.when(s > 0)(lambda which=which: every(halo_s.at[which], rel_send.at[which], c_recv).wait_send())


def per_device(grid, activations, filters, cotangent):
    micro, planes, C, cells = activations.shape[1:]
    nz, ny, nc = grid
    chunks = nz * ny * nc
    rows = -(-(27 * C * C) // (128 * 8 * chunks)) * 8
    rows = next(r for r in (8, 16, 32, 48, 96, 144, 288) if r >= rows)
    dma = pltpu.SemaphoreType.DMA
    vmem = pl.BlockSpec(memory_space=pltpu.VMEM)
    plane = (C, cells)
    return pl.pallas_call(
        functools.partial(kernel, grid),
        out_shape=(
            jax.ShapeDtypeStruct(activations.shape, F32),
            jax.ShapeDtypeStruct(filters.shape, F32),
        ),
        in_specs=[pl.BlockSpec(memory_space=pltpu.HBM)] * 3,
        out_specs=(vmem, vmem),
        scratch_shapes=[
            pltpu.VMEM(activations.shape, F32),
            pltpu.VMEM(filters.shape, F32),
            pltpu.VMEM(cotangent.shape, F32),
            pltpu.VMEM((9 * C, 8 * C), BF16),
            pltpu.VMEM((9 * C, 8 * C), BF16),
            pltpu.VMEM((2, micro, *plane), F32),
            pltpu.VMEM((2, micro, *plane), F32),
            pltpu.VMEM((micro, 10 * C, cells), BF16),
            pltpu.VMEM((micro, 10 * C, cells), BF16),
            pltpu.VMEM((2, 9 * C, cells), F32),
            pltpu.VMEM((micro, planes, *plane), F32),
            pltpu.VMEM((micro, planes, *plane), F32),
            pltpu.VMEM((micro, planes, *plane), F32),
            pltpu.VMEM((2, 9 * C, 2 * cells), BF16),
            pltpu.VMEM((9 * C, 3 * C), F32),
            pltpu.VMEM((chunks, rows, 128), F32),
            pltpu.VMEM((nz * ny, rows, 128), F32),
            pltpu.VMEM((max(ny - 1, 1), nz, rows, 128), F32),
            pltpu.VMEM((max(nz - 1, 1), rows, 128), F32),
            pltpu.VMEM((chunks, rows, 128), F32),
            dma((2,)), dma((2, micro)), dma((2,)), dma((2, micro)), dma((2,)), dma((2, micro)),
            dma, dma, dma, dma((ny - 1, nz)), dma, dma, dma, dma((nz - 1,)), dma, dma((ny - 1,)), dma, dma, dma((3,)),
            pltpu.SemaphoreType.REGULAR((3,)),
        ],
        compiler_params=pltpu.CompilerParams(
            collective_id=0, has_side_effects=True, vmem_limit_bytes=32 * 1024 * 1024
        ),
    )(*(pltpu.with_memory_space_constraint(x, pltpu.HBM) for x in (activations, filters, cotangent)))


def solution(mesh):
    slabs = mesh.shape["depth"]
    grid = (slabs // 8, 4, 2) if slabs >= 32 else (slabs // 4, 2, 2)
    return jax.shard_map(
        functools.partial(per_device, grid),
        mesh=mesh,
        in_specs=(
            P("section", None, "depth", None, None),
            P("section", None, None, None),
            P(None, "depth", None, None),
        ),
        out_specs=(P("section", None, "depth", None, None), P("section", None, None, None)),
        check_vma=False,
    )
```
